32 devices in a mesh: grp: 4 (over y, x), dev: 8 (over z, core).
Axes of the slice: x: 2, y: 2, z: 4, core: 2. Of those that a mesh axis runs over, the one named last changes fastest.
Arguments:
- table: bfloat16 [8, 32768, 256], P('grp', 'dev'), may hold values from -0.75 to 0.75
- token_ids: int32 [8192], P(('grp', 'dev')), may hold values from 0 to 32767, as said below
- hidden: bfloat16 [8192, 2560], P(('grp', 'dev')), may hold values from -6 to 6
- w_proj: bfloat16 [2560, 2048], replicated, may hold values from -0.125 to 0.125
- norm_gain: float32 [256], replicated, may hold values from 0.5 to 1.5
Outputs:
- served_table: bfloat16 [8, 4, 1024, 2048], P('dev', 'grp')
- layer_inputs: bfloat16 [8192, 8, 256], P(('grp', 'dev'))
The draws below stay inside these ranges and needn't reach their ends.
Inputs may be any that keep to these rules, and one draw needn't show every extreme that they name: `token_ids`: of the 256 tokens of one device, at most 16 have ids in any one aligned block of 1024 vocabulary rows, and exactly 16 in some block.
All inputs are finite; a program needn't handle non-finite values.
Results may differ from the reference program's by a relative error of at most 0.001.
Values may be sent and summed in bfloat16 or wider, within the bound.
A program may use at most 128 MiB of HBM per device.

```python
import math
import jax
import jax.numpy as jnp
from jax import lax

D = 2560
E = 256
LAYERS = 8
ROWS_DEV = 1024
TOK_DEV = 256
CAP = 16
VOCAB = 32768
TOKENS = 8192
N_GRP = 4
N_DEV = 8


def draw_token_ids(key, part):
    blocks = VOCAB // ROWS_DEV
    slots = blocks * CAP
    ranking = jax.random.permutation(jax.random.fold_in(key, 7), blocks).astype(jnp.int32)
    hotness = (ranking < max(blocks // 8, 1)).astype(jnp.int32)
    slot_ids = jnp.arange(slots, dtype=jnp.int32)
    slot_block = slot_ids // CAP

    def one_device(dev_key):
        key_full, key_score, key_order, key_first, key_second = jax.random.split(dev_key, 5)
        full_block = jax.random.randint(key_full, (), 0, blocks, dtype=jnp.int32)
        score = jax.random.randint(key_score, (slots,), 0, slots, dtype=jnp.int32) * slots + slot_ids
        score = score + jnp.take(hotness, slot_block) * slots * slots
        score = score + (slot_block == full_block).astype(jnp.int32) * 2 * slots * slots
        top_scores, chosen = lax.top_k(score, TOK_DEV)
        owners = (chosen.astype(jnp.int32) // CAP).astype(jnp.int32)
        order = jax.random.permutation(key_order, TOK_DEV)
        owners = owners[order]
        first = jax.random.randint(key_first, (TOK_DEV,), 0, ROWS_DEV, dtype=jnp.int32)
        second = jax.random.randint(key_second, (TOK_DEV,), 0, ROWS_DEV, dtype=jnp.int32)
        return owners * ROWS_DEV + jnp.minimum(first, second)
    dev_keys = jax.random.split(jax.random.fold_in(key, 11), blocks)
    return jax.vmap(one_device)(dev_keys).reshape(TOKENS).astype(jnp.int32)


def block_levels(stream_key, dims, pieces, low, top_value):
    loudness, own = 1.0, jax.random.fold_in(stream_key, 6)
    for position, parts in pieces:
        steps = jnp.exp(jax.random.uniform(jax.random.fold_in(own, position), (parts,), jnp.float32, low / len(pieces), top_value / len(pieces)))
        loudness = loudness * jnp.repeat(steps, dims[position] // parts).reshape([-1 if axis == position else 1 for axis in range(len(dims))])
    return loudness


def bell_draw(rng, extent, width, most, cuts=(), held_as=jnp.bfloat16):
    drawn = jax.random.normal(rng, extent, jnp.float32) * width
    if len(cuts) > 0:
        drawn = block_levels(rng, extent, cuts, -0.22, 0.18) * drawn
    return jnp.clip(drawn, min=-most, max=most).astype(held_as)


def setup_inputs(seed: int = 0) -> dict:
    seeds = jax.random.split(jax.random.key(seed), 6)
    table = bell_draw(seeds[0], (LAYERS, VOCAB, E), 0.125, 0.75, ((0, 4), (1, 8)))
    token_ids = draw_token_ids(jax.random.fold_in(seeds[5], 71), 0)
    hidden = bell_draw(seeds[2], (TOKENS, D), 1.0, 6.0, ((0, 32),))
    w_proj = bell_draw(seeds[3], (D, LAYERS * E), D ** -0.5, 0.125)
    norm_gain = jnp.clip(1.0 + 0.1 * jax.random.normal(seeds[4], (E,), jnp.float32), 0.5, 1.5)
    return dict(table=table, token_ids=token_ids, hidden=hidden, w_proj=w_proj, norm_gain=norm_gain)


def reference(table, token_ids, hidden, w_proj, norm_gain):
    served_table = jnp.transpose(table, (1, 0, 2)).reshape(N_DEV, N_GRP, ROWS_DEV, LAYERS * E)
    emb = jnp.transpose(jnp.take(table, token_ids, axis=1), (1, 0, 2)).astype(jnp.float32)
    proj = jnp.dot(hidden, w_proj, preferred_element_type=jnp.float32).reshape(TOKENS, LAYERS, E)
    mean_sq = lax.optimization_barrier(jnp.mean(proj * proj, axis=-1, keepdims=True))
    normed = proj / jnp.sqrt(mean_sq + 1e-06) * norm_gain
    layer_inputs = ((normed + math.sqrt(E) * emb) / math.sqrt(2.0)).astype(jnp.bfloat16)
    return (served_table, layer_inputs)
```

```python
import functools
import math

import jax
import jax.numpy as jnp
from jax import lax
from jax.experimental import pallas as pl
from jax.experimental.pallas import tpu as pltpu
from jax.sharding import PartitionSpec as P

MESH = pl.DeviceIdType.MESH
LANES = 128
PIECES = 8
SPLIT = (10, 12, 14)


def column(row):
    return jnp.transpose(jnp.broadcast_to(row, (LANES, LANES)))


def exchange(n_grp, n_dev, cap,
             ids_hbm, hidden_hbm, gain_hbm, table_ref, w_ref,
             served_ref, out_ref,
             ids_ref, hidden_ref, gain_ref, tbl, wbuf, want_buf, req_send, req_buf, merged,
             send, recv, esend, erecv, mix,
             want_ss, want_rs, req_ss, req_rs, mrg_ss, mrg_rs, tab_ss, tab_rs, z_ss, z_rs, e_ss, e_rs,
             ids_sem, tbl_sem, w_sem, hidden_sem, gain_sem, own_sem):
    g = lax.axis_index("grp")
    d = lax.axis_index("dev")
    layer_share, vocab_share, width = table_ref.shape
    rows = vocab_share // n_grp
    tok = hidden_ref.shape[0]
    halves = tok // LANES
    layers = layer_share * n_grp
    blocks = n_grp * n_dev
    slots = n_grp * cap
    all_slots = n_dev * slots
    groups = n_dev * cap // LANES
    half_grp = n_grp // 2
    f32 = jnp.float32
    bf16 = jnp.bfloat16

    def grp_at(i):
        return lax.rem(g // 2 + i // 2, half_grp) * 2 + lax.rem(g % 2 + i % 2, 2)

    def back(i):
        return ((half_grp - i // 2) % half_grp) * 2 + i % 2

    def dev_at(j):
        return lax.rem(d + j, n_dev)

    def to_grp(i):
        return dict(device_id={"grp": grp_at(i), "dev": d}, device_id_type=MESH)

    def to_dev(j):
        return dict(device_id={"grp": g, "dev": dev_at(j)}, device_id_type=MESH)

    order = list(range(n_grp - 1, -1, -1))

    barrier = pltpu.get_barrier_semaphore()
    for i in range(1, n_grp):
        pl.semaphore_signal(barrier, inc=1, **to_grp(i))

    def greet(j, carry):
        pl.semaphore_signal(barrier, inc=1, **to_dev(j))
        return carry
    lax.fori_loop(1, n_dev, greet, 0)

    load_ids = pltpu.make_async_copy(ids_hbm, ids_ref, ids_sem)
    load_ids.start()
    load_table = pltpu.make_async_copy(table_ref, tbl, tbl_sem)
    load_table.start()
    load_w = pltpu.make_async_copy(w_ref, wbuf, w_sem)
    load_w.start()
    load_hidden = pltpu.make_async_copy(hidden_hbm, hidden_ref, hidden_sem)
    load_hidden.start()
    load_gain = pltpu.make_async_copy(gain_hbm, gain_ref, gain_sem)
    load_gain.start()

    part = rows // PIECES
    pieces = [(l, p) for l in range(layer_share) for p in range(PIECES)]

    def tab_copy(i, l, p):
        gp = grp_at(i)
        return pltpu.make_async_remote_copy(
            src_ref=table_ref.at[l, pl.ds(pl.multiple_of(gp * rows + p * part, part), part), :],
            dst_ref=served_ref.at[
                pl.ds(p * part, part),
                pl.ds(pl.multiple_of((g * layer_share + l) * width, width), width),
            ],
            send_sem=tab_ss.at[i, l, p], recv_sem=tab_rs.at[i, l, p], **to_grp(i),
        )

    cuts = [0] + [len(pieces) * s // 16 for s in SPLIT] + [len(pieces)]

    def start_pieces(k):
        for l, p in pieces[cuts[k]:cuts[k + 1]]:
            for i in range(n_grp - 1, 0, -1):
                tab_copy(i, l, p).start()

    def own_copy(l):
        return pltpu.make_async_copy(
            table_ref.at[l, pl.ds(pl.multiple_of(g * rows, rows), rows), :],
            served_ref.at[:, pl.ds(pl.multiple_of((g * layer_share + l) * width, width), width)],
            own_sem.at[l],
        )

    pl.semaphore_wait(barrier, n_grp - 1 + n_dev - 1)
    start_pieces(0)

    load_ids.wait()
    lane = lax.broadcasted_iota(jnp.int32, (LANES, LANES), 1).astype(f32)
    sub = lax.broadcasted_iota(jnp.int32, (LANES, LANES), 0).astype(f32)
    id_row = [ids_ref[h:h + 1, :].astype(f32) for h in range(halves)]
    id_col = [column(r) for r in id_row]

    def owner_of(v):
        return jnp.floor((v + 0.5) * (1.0 / rows))

    own_row = [owner_of(r) for r in id_row]
    own_col = [owner_of(c) for c in id_col]
    slot_col = []
    for h in range(halves):
        by_lane = jnp.zeros((LANES, LANES), f32)
        by_sub = jnp.zeros((LANES, LANES), f32)
        for k in range(h + 1):
            same = own_col[h] == own_row[k]
            also = own_col[k] == own_row[h]
            if k == h:
                same = same & (lane < sub)
                also = also & (sub < lane)
            by_lane = by_lane + jnp.where(same, 1.0, 0.0)
            by_sub = by_sub + jnp.where(also, 1.0, 0.0)
        slot_col.append(jnp.sum(by_lane, axis=1, keepdims=True))
        want_buf[g, h:h + 1, :] = own_row[h] * cap + jnp.sum(by_sub, axis=0, keepdims=True)

    block_id = lax.broadcasted_iota(jnp.int32, (blocks, LANES), 0).astype(f32)
    chooser = jnp.concatenate(
        [jnp.where(own_row[h] == block_id, 1.0, 0.0).astype(bf16) for h in range(halves)], axis=1
    )
    base = (d * cap).astype(f32)
    for r in range(groups):
        high, low = [], []
        for h in range(halves):
            at_slot = slot_col[h] == lane + (r * LANES) - base
            local = id_col[h] - own_col[h] * rows
            hi = jnp.floor(local * (1.0 / 256.0))
            high.append(jnp.where(at_slot, hi, 0.0).astype(bf16))
            low.append(jnp.where(at_slot, local - hi * 256.0 + 1.0, 0.0).astype(bf16))
        ask = jnp.dot(chooser, jnp.concatenate(high, axis=0), preferred_element_type=f32) * 256.0
        ask = ask + jnp.dot(chooser, jnp.concatenate(low, axis=0), preferred_element_type=f32)
        req_send[:, :, r * LANES:(r + 1) * LANES] = ask.reshape(n_dev, n_grp, LANES)

    def req_copy(j):
        return pltpu.make_async_remote_copy(
            src_ref=req_send.at[dev_at(j)], dst_ref=req_buf.at[d],
            send_sem=req_ss.at[j], recv_sem=req_rs.at[j], **to_dev(j),
        )

    def start_req(j, carry):
        req_copy(j).start()
        return carry
    lax.fori_loop(1, n_dev, start_req, 0)

    def want_copy(i):
        return pltpu.make_async_remote_copy(
            src_ref=want_buf.at[g], dst_ref=want_buf.at[g],
            send_sem=want_ss.at[i], recv_sem=want_rs.at[i], **to_grp(i),
        )

    for i in range(1, n_grp):
        want_copy(i).start()

    for l in range(layer_share):
        own_copy(l).start()

    req_buf[d] = req_send[d]

    def take_req(j, carry):
        req_copy(j).wait_recv()
        return carry
    lax.fori_loop(1, n_dev, take_req, 0)
    total = req_buf[0]
    for a in range(1, n_dev):
        total = total + req_buf[a]
    for b in range(n_grp):
        merged[g, b] = total[b:b + 1, :]

    def mrg_copy(i):
        return pltpu.make_async_remote_copy(
            src_ref=merged.at[g], dst_ref=merged.at[g],
            send_sem=mrg_ss.at[i], recv_sem=mrg_rs.at[i], **to_grp(i),
        )

    for i in range(n_grp - 1, 0, -1):
        mrg_copy(i).start()
    load_table.wait()

    def z_copy(o, j):
        dp = dev_at(j)
        gp = grp_at(o)
        return pltpu.make_async_remote_copy(
            src_ref=send.at[o, dp],
            dst_ref=recv.at[gp, pl.ds(pl.multiple_of(d * slots, slots), slots), :],
            send_sem=z_ss.at[o, j], recv_sem=z_rs.at[o, j], **to_dev(j),
        )

    spread = LANES // cap
    for o in order:
        gp = grp_at(o)
        if o:
            mrg_copy(back(o)).wait_recv()

        def block(b, carry, o=o, gp=gp):
            at = pl.multiple_of(b * cap, cap)
            for r in range(groups):
                wanted = column(merged[gp, b, :, r * LANES:(r + 1) * LANES]) - (lane + 1.0)
                hit = jnp.concatenate(
                    [(wanted == float(c * LANES)).astype(f32) for c in range(rows // LANES)], axis=1
                ).astype(bf16)
                for l in range(layer_share):
                    found = jnp.dot(
                        hit, tbl[l, pl.ds(pl.multiple_of(b * rows, rows), rows), :],
                        preferred_element_type=f32,
                    ).astype(bf16)
                    send[o, r * spread:(r + 1) * spread, pl.ds(at, cap), l * width:(l + 1) * width] = (
                        found.reshape(spread, cap, width)
                    )
            return carry
        lax.fori_loop(0, n_grp, block, 0)

        def start_z(j, carry, o=o):
            z_copy(o, j).start()
            return carry
        lax.fori_loop(1, n_dev, start_z, 0)
        recv[gp, pl.ds(pl.multiple_of(d * slots, slots), slots), :] = send[o, d]

    load_w.wait()
    load_hidden.wait()
    load_gain.wait()

    def project(l):
        proj = jnp.dot(hidden_ref[...], wbuf[:, l * width:(l + 1) * width], preferred_element_type=f32)
        mean_sq = jnp.mean(proj * proj, axis=-1, keepdims=True)
        return proj / jnp.sqrt(mean_sq + 1e-06) * gain_ref[...]

    for l in range(layers):
        mix[:, l, :] = project(l)

    def e_copy(o):
        return pltpu.make_async_remote_copy(
            src_ref=esend.at[o], dst_ref=erecv.at[g],
            send_sem=e_ss.at[o], recv_sem=e_rs.at[o], **to_grp(o),
        )

    for step, o in enumerate(order):
        gp = grp_at(o)
        if o:
            want_copy(back(o)).wait_recv()
        pickers = []
        for t in range(halves):
            mine = column(want_buf[gp, t:t + 1, :]) - lane
            pickers.append(jnp.concatenate(
                [(mine == float(c * LANES)).astype(f32) for c in range(all_slots // LANES)], axis=1
            ).astype(bf16))

        def take_rows(j, carry, o=o):
            z_copy(o, j).wait_recv()
            return carry
        lax.fori_loop(1, n_dev, take_rows, 0)

        for t in range(halves):
            picked = jnp.dot(pickers[t], recv[gp], preferred_element_type=f32).astype(bf16)
            if o:
                esend[o, t * LANES:(t + 1) * LANES, :] = picked
            else:
                erecv[g, t * LANES:(t + 1) * LANES, :] = picked
        if o:
            e_copy(o).start()
        if step < len(SPLIT):
            start_pieces(step + 1)

    for o in range(1, n_grp):
        e_copy(o).wait_recv()

    for l in range(layers):
        at = (l % layer_share) * width
        emb = erecv[l // layer_share, :, at:at + width].astype(f32)
        mix[:, l, :] = (mix[:, l, :] + math.sqrt(width) * emb) / math.sqrt(2.0)
    out_ref[...] = mix[...].astype(bf16)

    for l in range(layer_share):
        own_copy(l).wait()
    for i in range(1, n_grp):
        want_copy(i).wait_send()
        mrg_copy(i).wait_send()
        e_copy(i).wait_send()

    def end_dev(j, carry):
        req_copy(j).wait_send()
        for o in range(n_grp):
            z_copy(o, j).wait_send()
        return carry
    lax.fori_loop(1, n_dev, end_dev, 0)
    for l, p in pieces:
        for i in range(1, n_grp):
            tab_copy(i, l, p).wait()


def put_out(served_ref, mixed_ref, served_hbm, mixed_hbm, sems):
    parts = sems.shape[0] - 1
    span = served_ref.shape[0] // parts
    copies = [
        pltpu.make_async_copy(
            served_ref.at[pl.ds(k * span, span), :], served_hbm.at[pl.ds(k * span, span), :], sems.at[k]
        )
        for k in range(parts)
    ]
    copies.append(pltpu.make_async_copy(mixed_ref, mixed_hbm, sems.at[parts]))
    for copy in copies:
        copy.start()
    for copy in copies:
        copy.wait()


def on_device(table, token_ids, hidden, w_proj, norm_gain):
    n_grp = lax.axis_size("grp")
    n_dev = lax.axis_size("dev")
    layer_share, vocab_share, width = table.shape
    layers = layer_share * n_grp
    tok = token_ids.shape[0]
    rows = vocab_share // n_grp
    blocks = n_grp * n_dev
    cap = -(-max(2, 2 * tok // blocks) // 16) * 16
    slots = n_grp * cap
    lanes = n_dev * cap
    assert n_grp % 2 == 0 and lanes % LANES == 0 and tok % LANES == 0 and rows % LANES == 0
    wide = layer_share * width

    vmem = pl.BlockSpec(memory_space=pltpu.VMEM)
    hbm = pl.BlockSpec(memory_space=pltpu.HBM)
    dma = pltpu.SemaphoreType.DMA
    bf16 = jnp.bfloat16
    f32 = jnp.float32
    served, mixed = pl.pallas_call(
        functools.partial(exchange, n_grp, n_dev, cap),
        out_shape=(
            pltpu.VMEM((rows, layers * width), bf16),
            pltpu.VMEM((tok, layers, width), bf16),
        ),
        in_specs=[hbm] * 5,
        out_specs=(vmem, vmem),
        scratch_shapes=[
            pltpu.VMEM((tok // LANES, LANES), jnp.int32),
            pltpu.VMEM(hidden.shape, bf16),
            pltpu.VMEM((1, width), f32),
            pltpu.VMEM(table.shape, bf16),
            pltpu.VMEM(w_proj.shape, bf16),
            pltpu.VMEM((n_grp, tok // LANES, LANES), f32),
            pltpu.VMEM((n_dev, n_grp, lanes), f32),
            pltpu.VMEM((n_dev, n_grp, lanes), f32),
            pltpu.VMEM((n_grp, n_grp, 1, lanes), f32),
            pltpu.VMEM((n_grp, n_dev, slots, wide), bf16),
            pltpu.VMEM((n_grp, n_dev * slots, wide), bf16),
            pltpu.VMEM((n_grp, tok, wide), bf16),
            pltpu.VMEM((n_grp, tok, wide), bf16),
            pltpu.VMEM((tok, layers, width), f32),
            dma((n_grp,)), dma((n_grp,)),
            dma((n_dev,)), dma((n_dev,)),
            dma((n_grp,)), dma((n_grp,)),
            dma((n_grp, layer_share, PIECES)), dma((n_grp, layer_share, PIECES)),
            dma((n_grp, n_dev)), dma((n_grp, n_dev)),
            dma((n_grp,)), dma((n_grp,)),
            dma, dma, dma, dma, dma, dma((layer_share,)),
        ],
        compiler_params=pltpu.CompilerParams(
            collective_id=0, has_side_effects=True, vmem_limit_bytes=58 * 2**20
        ),
        name="exchange",
    )(token_ids.reshape(tok // LANES, LANES), hidden, norm_gain.reshape(1, width), table, w_proj)
    served, mixed = pl.pallas_call(
        put_out,
        out_shape=(
            jax.ShapeDtypeStruct(served.shape, bf16),
            jax.ShapeDtypeStruct(mixed.shape, bf16),
        ),
        in_specs=[vmem, vmem],
        out_specs=(hbm, hbm),
        scratch_shapes=[dma((9,))],
        compiler_params=pltpu.CompilerParams(vmem_limit_bytes=2 * 2**20),
        name="put_out",
    )(served, mixed)
    return (served.reshape(1, 1, rows, layers * width), mixed)


def solution(mesh):
    in_specs = (P("grp", "dev", None), P(("grp", "dev")), P(("grp", "dev"), None), P(), P())
    out_specs = (P("dev", "grp", None, None), P(("grp", "dev"), None, None))
    return jax.shard_map(
        on_device, mesh=mesh, in_specs=in_specs, out_specs=out_specs, check_vma=False
    )
```

```python
import functools
import math

import jax
import jax.numpy as jnp
from jax import lax
from jax.experimental import pallas as pl
from jax.experimental.pallas import tpu as pltpu
from jax.sharding import PartitionSpec as P

MESH = pl.DeviceIdType.MESH
LANES = 128
PIECES = 8
SPLIT = (11, 13, 15)
OWN_FIRST = 1


def column(row):
    return jnp.transpose(jnp.broadcast_to(row, (LANES, LANES)))


def exchange(n_grp, n_dev, cap,
             ids_hbm, hidden_hbm, gain_hbm, table_ref, w_ref,
             served_ref, out_ref,
             ids_buf, hidden_ref, gain_ref, tbl, wbuf, want, req_own, req_oth, buf_own, buf_oth, merged,
             send, recv, esend, erecv, mix,
             ids_ss, ids_rs, req_ss, req_rs, tab_ss, tab_rs, z_ss, z_rs, e_ss, e_rs,
             in_grp, in_dev, ids_sem, tbl_sem, w_sem, hidden_sem, gain_sem, own_sem):
    g = lax.axis_index("grp")
    d = lax.axis_index("dev")
    layer_share, vocab_share, width = table_ref.shape
    rows = vocab_share // n_grp
    tok = hidden_ref.shape[0]
    halves = tok // LANES
    layers = layer_share * n_grp
    blocks = n_grp * n_dev
    slots = n_grp * cap
    all_slots = n_dev * slots
    groups = n_dev * cap // LANES
    half_grp = n_grp // 2
    req_send = (req_own, req_oth)
    req_buf = (buf_own, buf_oth)
    f32 = jnp.float32
    bf16 = jnp.bfloat16

    def grp_at(i):
        return lax.rem(g // 2 + i // 2, half_grp) * 2 + lax.rem(g % 2 + i % 2, 2)

    def back(i):
        return ((half_grp - i // 2) % half_grp) * 2 + i % 2

    def dev_at(j):
        return lax.rem(d + j, n_dev)

    def to_grp(i):
        return dict(device_id={"grp": grp_at(i), "dev": d}, device_id_type=MESH)

    def to_dev(j):
        return dict(device_id={"grp": g, "dev": dev_at(j)}, device_id_type=MESH)

    barrier = pltpu.get_barrier_semaphore()
    for i in range(1, n_grp):
        @pl.when(grp_at(i) > g)
        def _(i=i):
            pl.semaphore_signal(barrier, inc=1, **to_grp(i))

    def greet(j, carry):
        pl.semaphore_signal(barrier, inc=1, **to_dev(j))
        return carry
    lax.fori_loop(1, n_dev - d, greet, 0)

    load_ids = pltpu.make_async_copy(ids_hbm, ids_buf.at[g], ids_sem)
    load_ids.start()
    load_table = pltpu.make_async_copy(table_ref, tbl, tbl_sem)
    load_table.start()
    load_w = pltpu.make_async_copy(w_ref, wbuf, w_sem)
    load_w.start()
    load_hidden = pltpu.make_async_copy(hidden_hbm, hidden_ref, hidden_sem)
    load_hidden.start()
    load_gain = pltpu.make_async_copy(gain_hbm, gain_ref, gain_sem)
    load_gain.start()

    part = rows // PIECES
    pieces = [(l, p) for l in range(layer_share) for p in range(PIECES)]

    def tab_copy(i, l, p):
        gp = grp_at(i)
        return pltpu.make_async_remote_copy(
            src_ref=table_ref.at[l, pl.ds(pl.multiple_of(gp * rows + p * part, part), part), :],
            dst_ref=served_ref.at[
                pl.ds(p * part, part),
                pl.ds(pl.multiple_of((g * layer_share + l) * width, width), width),
            ],
            send_sem=tab_ss.at[i, l, p], recv_sem=tab_rs.at[i, l, p], **to_grp(i),
        )

    cuts = [1] + [len(pieces) * s // 16 for s in SPLIT] + [len(pieces)]

    def start_pieces(k):
        for l, p in pieces[cuts[k]:cuts[k + 1]] if k <= len(SPLIT) else ():
            for i in range(n_grp - 1, 0, -1):
                tab_copy(i, l, p).start()

    def own_copy(l):
        return pltpu.make_async_copy(
            table_ref.at[l, pl.ds(pl.multiple_of(g * rows, rows), rows), :],
            served_ref.at[:, pl.ds(pl.multiple_of((g * layer_share + l) * width, width), width)],
            own_sem.at[l],
        )

    def ids_copy(i):
        return pltpu.make_async_remote_copy(
            src_ref=ids_buf.at[g], dst_ref=ids_buf.at[g],
            send_sem=ids_ss.at[i], recv_sem=ids_rs.at[i], **to_grp(i),
        )

    @pl.when(g + d > 0)
    def _():
        pl.semaphore_wait(barrier, g + d)
    for i in range(1, n_grp):
        @pl.when(grp_at(i) < g)
        def _(i=i):
            pl.semaphore_signal(in_grp.at[back(i)], inc=1, **to_grp(i))

    def reply(j, carry):
        pl.semaphore_signal(in_dev, inc=1, **to_dev(j))
        return carry
    lax.fori_loop(n_dev - d, n_dev, reply, 0)

    load_ids.wait()
    for i in range(1, n_grp):
        @pl.when(grp_at(i) > g)
        def _(i=i):
            pl.semaphore_wait(in_grp.at[i], 1)
        ids_copy(i).start()
        l, p = pieces[0]
        tab_copy(i, l, p).start()
    start_pieces(0)
    for l in range(layer_share):
        own_copy(l).start()

    lane = lax.broadcasted_iota(jnp.int32, (LANES, LANES), 1).astype(f32)
    sub = lax.broadcasted_iota(jnp.int32, (LANES, LANES), 0).astype(f32)
    block_id = lax.broadcasted_iota(jnp.int32, (blocks, LANES), 0).astype(f32)
    base = (d * cap).astype(f32)

    def owner_of(v):
        return jnp.floor((v + 0.5) * (1.0 / rows))

    def ask_for(o, req, row):
        gp = grp_at(o)
        id_row = [ids_buf[gp, h:h + 1, :].astype(f32) for h in range(halves)]
        id_col = [column(v) for v in id_row]
        own_row = [owner_of(v) for v in id_row]
        own_col = [owner_of(v) for v in id_col]
        slot_col = []
        for h in range(halves):
            earlier = jnp.zeros((LANES, LANES), f32)
            for k in range(h + 1):
                same = own_col[h] == own_row[k]
                if k == h:
                    same = same & (lane < sub)
                earlier = earlier + jnp.where(same, 1.0, 0.0)
            slot_col.append(jnp.sum(earlier, axis=1, keepdims=True))
            want[o, h] = own_col[h] * cap + slot_col[h]
        chooser = jnp.concatenate(
            [jnp.where(own_row[h] == block_id, 1.0, 0.0).astype(bf16) for h in range(halves)], axis=1
        )
        for r in range(groups):
            high, low = [], []
            for h in range(halves):
                at_slot = slot_col[h] == lane + (r * LANES) - base
                local = id_col[h] - own_col[h] * rows
                hi = jnp.floor(local * (1.0 / 256.0))
                high.append(jnp.where(at_slot, hi, 0.0).astype(bf16))
                low.append(jnp.where(at_slot, local - hi * 256.0 + 1.0, 0.0).astype(bf16))
            ask = jnp.dot(chooser, jnp.concatenate(high, axis=0), preferred_element_type=f32) * 256.0
            ask = ask + jnp.dot(chooser, jnp.concatenate(low, axis=0), preferred_element_type=f32)
            req[:, row:row + n_grp, r * LANES:(r + 1) * LANES] = (
                ask.reshape(n_dev, n_grp, LANES)
            )

    def req_copy(k, j):
        return pltpu.make_async_remote_copy(
            src_ref=req_send[k].at[dev_at(j)], dst_ref=req_buf[k].at[d],
            send_sem=req_ss.at[k, j], recv_sem=req_rs.at[k, j], **to_dev(j),
        )

    def start_req(k):
        def body(j, carry):
            req_copy(k, j).start()
            return carry
        lax.fori_loop(1, n_dev, body, 0)
        req_buf[k][d] = req_send[k][d]

    def take_req(k):
        def body(j, carry):
            req_copy(k, j).wait_recv()
            return carry
        lax.fori_loop(1, n_dev, body, 0)
        total = req_buf[k][0]
        for a in range(1, n_dev):
            total = total + req_buf[k][a]
        return total

    ask_for(0, req_send[0], 0)
    @pl.when(d < n_dev - 1)
    def _():
        pl.semaphore_wait(in_dev, n_dev - 1 - d)
    start_req(0)
    for o in range(1, n_grp):
        ids_copy(back(o)).wait_recv()
    for o in range(1, n_grp):
        ask_for(o, req_send[1], (o - 1) * n_grp)
    start_req(1)

    first = max(1, n_grp * OWN_FIRST // 4)
    phases = [(0, 0, first)] + [(o, 0, n_grp) for o in range(n_grp - 1, 0, -1)] + [(0, first, n_grp)]

    def z_copy(f, j):
        o, lo, hi = phases[f]
        span = (hi - lo) * cap
        return pltpu.make_async_remote_copy(
            src_ref=send.at[o, dev_at(j), lo * cap:hi * cap],
            dst_ref=recv.at[grp_at(o), pl.ds(pl.multiple_of(d * slots + lo * cap, cap), span), :],
            send_sem=z_ss.at[f, j], recv_sem=z_rs.at[f, j], **to_dev(j),
        )

    spread = LANES // cap
    total = take_req(0)
    for b in range(n_grp):
        merged[0, b] = total[b:b + 1, :]
    load_table.wait()
    for f, (o, lo, hi) in enumerate(phases):
        if f == 1:
            total = take_req(1)
            for k in range(n_grp, n_grp * n_grp):
                merged[k // n_grp, k % n_grp] = total[k - n_grp:k - n_grp + 1, :]

        def block(b, carry, o=o):
            at = pl.multiple_of(b * cap, cap)
            for r in range(groups):
                wanted = column(merged[o, b, :, r * LANES:(r + 1) * LANES]) - (lane + 1.0)
                hit = jnp.concatenate(
                    [(wanted == float(c * LANES)).astype(f32) for c in range(rows // LANES)], axis=1
                ).astype(bf16)
                for l in range(layer_share):
                    found = jnp.dot(
                        hit, tbl[l, pl.ds(pl.multiple_of(b * rows, rows), rows), :],
                        preferred_element_type=f32,
                    ).astype(bf16)
                    send[o, r * spread:(r + 1) * spread, pl.ds(at, cap), l * width:(l + 1) * width] = (
                        found.reshape(spread, cap, width)
                    )
            return carry
        lax.fori_loop(lo, hi, block, 0)

        def start_z(j, carry, f=f):
            z_copy(f, j).start()
            return carry
        lax.fori_loop(1, n_dev, start_z, 0)
        recv[grp_at(o), pl.ds(pl.multiple_of(d * slots + lo * cap, cap), (hi - lo) * cap), :] = (
            send[o, d, lo * cap:hi * cap]
        )

    load_w.wait()
    load_hidden.wait()
    load_gain.wait()

    def project(l):
        proj = jnp.dot(hidden_ref[...], wbuf[:, l * width:(l + 1) * width], preferred_element_type=f32)
        mean_sq = jnp.mean(proj * proj, axis=-1, keepdims=True)
        return proj / jnp.sqrt(mean_sq + 1e-06) * gain_ref[...]

    for l in range(layers):
        mix[:, l, :] = project(l)

    def e_copy(o):
        return pltpu.make_async_remote_copy(
            src_ref=esend.at[o], dst_ref=erecv.at[g],
            send_sem=e_ss.at[o], recv_sem=e_rs.at[o], **to_grp(o),
        )

    def take_rows(f):
        def body(j, carry):
            z_copy(f, j).wait_recv()
            return carry
        lax.fori_loop(1, n_dev, body, 0)

    def pickers(o):
        made = []
        for t in range(halves):
            mine = want[o, t] - lane
            made.append(jnp.concatenate(
                [(mine == float(c * LANES)).astype(f32) for c in range(all_slots // LANES)], axis=1
            ).astype(bf16))
        return made

    def pick(o, dst, at):
        for t, picker in enumerate(pickers(o)):
            dst[at, t * LANES:(t + 1) * LANES, :] = jnp.dot(
                picker, recv[grp_at(o)], preferred_element_type=f32
            ).astype(bf16)

    def add_rows(a):
        for k in range(layer_share):
            l = a * layer_share + k
            emb = erecv[a, :, k * width:(k + 1) * width].astype(f32)
            mix[:, l, :] = (mix[:, l, :] + math.sqrt(width) * emb) / math.sqrt(2.0)

    for f in range(1, n_grp):
        take_rows(f)
        pick(phases[f][0], esend, phases[f][0])
        e_copy(phases[f][0]).start()
        start_pieces(f)

    for o in range(1, n_grp):
        e_copy(o).wait_recv()
    for a in range(n_grp):
        @pl.when(g != a)
        def _(a=a):
            add_rows(a)
    take_rows(0)
    take_rows(n_grp)
    pick(0, erecv, g)
    for a in range(n_grp):
        @pl.when(g == a)
        def _(a=a):
            add_rows(a)
    out_ref[...] = mix[...].astype(bf16)

    for l in range(layer_share):
        own_copy(l).wait()
    for i in range(1, n_grp):
        ids_copy(i).wait_send()
        e_copy(i).wait_send()

    def end_dev(j, carry):
        for k in range(2):
            req_copy(k, j).wait_send()
        for f in range(n_grp + 1):
            z_copy(f, j).wait_send()
        return carry
    lax.fori_loop(1, n_dev, end_dev, 0)
    for l, p in pieces:
        for i in range(1, n_grp):
            tab_copy(i, l, p).wait()


def put_out(served_ref, mixed_ref, served_hbm, mixed_hbm, sems):
    parts = sems.shape[0] - 1
    span = served_ref.shape[0] // parts
    copies = [
        pltpu.make_async_copy(
            served_ref.at[pl.ds(k * span, span), :], served_hbm.at[pl.ds(k * span, span), :], sems.at[k]
        )
        for k in range(parts)
    ]
    copies.append(pltpu.make_async_copy(mixed_ref, mixed_hbm, sems.at[parts]))
    for copy in copies:
        copy.start()
    for copy in copies:
        copy.wait()


def on_device(table, token_ids, hidden, w_proj, norm_gain):
    n_grp = lax.axis_size("grp")
    n_dev = lax.axis_size("dev")
    layer_share, vocab_share, width = table.shape
    layers = layer_share * n_grp
    tok = token_ids.shape[0]
    rows = vocab_share // n_grp
    blocks = n_grp * n_dev
    cap = -(-max(2, 2 * tok // blocks) // 16) * 16
    slots = n_grp * cap
    lanes = n_dev * cap
    assert n_grp % 2 == 0 and lanes % LANES == 0 and tok % LANES == 0 and rows % LANES == 0
    wide = layer_share * width

    vmem = pl.BlockSpec(memory_space=pltpu.VMEM)
    hbm = pl.BlockSpec(memory_space=pltpu.HBM)
    dma = pltpu.SemaphoreType.DMA
    bf16 = jnp.bfloat16
    f32 = jnp.float32
    served, mixed = pl.pallas_call(
        functools.partial(exchange, n_grp, n_dev, cap),
        out_shape=(
            pltpu.VMEM((rows, layers * width), bf16),
            pltpu.VMEM((tok, layers, width), bf16),
        ),
        in_specs=[hbm] * 5,
        out_specs=(vmem, vmem),
        scratch_shapes=[
            pltpu.VMEM((n_grp, tok // LANES, LANES), jnp.int32),
            pltpu.VMEM(hidden.shape, bf16),
            pltpu.VMEM((1, width), f32),
            pltpu.VMEM(table.shape, bf16),
            pltpu.VMEM(w_proj.shape, bf16),
            pltpu.VMEM((n_grp, tok // LANES, LANES, LANES), f32),
            pltpu.VMEM((n_dev, n_grp, lanes), f32),
            pltpu.VMEM((n_dev, (n_grp - 1) * n_grp, lanes), f32),
            pltpu.VMEM((n_dev, n_grp, lanes), f32),
            pltpu.VMEM((n_dev, (n_grp - 1) * n_grp, lanes), f32),
            pltpu.VMEM((n_grp, n_grp, 1, lanes), f32),
            pltpu.VMEM((n_grp, n_dev, slots, wide), bf16),
            pltpu.VMEM((n_grp, n_dev * slots, wide), bf16),
            pltpu.VMEM((n_grp, tok, wide), bf16),
            pltpu.VMEM((n_grp, tok, wide), bf16),
            pltpu.VMEM((tok, layers, width), f32),
            dma((n_grp,)), dma((n_grp,)),
            dma((2, n_dev)), dma((2, n_dev)),
            dma((n_grp, layer_share, PIECES)), dma((n_grp, layer_share, PIECES)),
            dma((n_grp + 1, n_dev)), dma((n_grp + 1, n_dev)),
            dma((n_grp,)), dma((n_grp,)),
            pltpu.SemaphoreType.REGULAR((n_grp,)), pltpu.SemaphoreType.REGULAR,
            dma, dma, dma, dma, dma, dma((layer_share,)),
        ],
        compiler_params=pltpu.CompilerParams(
            collective_id=0, has_side_effects=True, vmem_limit_bytes=58 * 2**20
        ),
        name="exchange",
    )(token_ids.reshape(tok // LANES, LANES), hidden, norm_gain.reshape(1, width), table, w_proj)
    served, mixed = pl.pallas_call(
        put_out,
        out_shape=(
            jax.ShapeDtypeStruct(served.shape, bf16),
            jax.ShapeDtypeStruct(mixed.shape, bf16),
        ),
        in_specs=[vmem, vmem],
        out_specs=(hbm, hbm),
        scratch_shapes=[dma((9,))],
        compiler_params=pltpu.CompilerParams(vmem_limit_bytes=2 * 2**20),
        name="put_out",
    )(served, mixed)
    return (served.reshape(1, 1, rows, layers * width), mixed)


def solution(mesh):
    in_specs = (P("grp", "dev", None), P(("grp", "dev")), P(("grp", "dev"), None), P(), P())
    out_specs = (P("dev", "grp", None, None), P(("grp", "dev"), None, None))
    return jax.shard_map(
        on_device, mesh=mesh, in_specs=in_specs, out_specs=out_specs, check_vma=False
    )
```

```python
import functools
import math

import jax
import jax.numpy as jnp
from jax import lax
from jax.experimental import pallas as pl
from jax.experimental.pallas import tpu as pltpu
from jax.sharding import PartitionSpec as P

MESH = pl.DeviceIdType.MESH
LANES = 128
PIECES = 8
SPLIT = (12, 14, 15)
OWN_FIRST = 1
AHEAD = 2


def column(row):
    return jnp.transpose(jnp.broadcast_to(row, (LANES, LANES)))


def exchange(n_grp, n_dev, cap,
             ids_hbm, hidden_hbm, gain_hbm, table_ref, w_ref,
             served_ref, out_ref,
             ids_buf, hidden_ref, gain_ref, tbl, wbuf, want, req_own, req_oth, buf_own, buf_oth, merged,
             send, recv, esend, erecv, mix,
             ids_ss, ids_rs, req_ss, req_rs, tab_ss, tab_rs, z_ss, z_rs, e_ss, e_rs,
             in_grp, in_dev, ids_sem, tbl_sem, w_sem, hidden_sem, gain_sem, own_sem):
    g = lax.axis_index("grp")
    d = lax.axis_index("dev")
    layer_share, vocab_share, width = table_ref.shape
    rows = vocab_share // n_grp
    tok = hidden_ref.shape[0]
    halves = tok // LANES
    layers = layer_share * n_grp
    blocks = n_grp * n_dev
    slots = n_grp * cap
    all_slots = n_dev * slots
    groups = n_dev * cap // LANES
    half_grp = n_grp // 2
    req_send = (req_own, req_oth)
    req_buf = (buf_own, buf_oth)
    f32 = jnp.float32
    bf16 = jnp.bfloat16

    def grp_at(i):
        return lax.rem(g // 2 + i // 2, half_grp) * 2 + lax.rem(g % 2 + i % 2, 2)

    def back(i):
        return ((half_grp - i // 2) % half_grp) * 2 + i % 2

    def dev_at(j):
        return lax.rem(d + j, n_dev)

    def to_grp(i):
        return dict(device_id={"grp": grp_at(i), "dev": d}, device_id_type=MESH)

    def to_dev(j):
        return dict(device_id={"grp": g, "dev": dev_at(j)}, device_id_type=MESH)

    def drain(part, sem):
        pltpu.make_async_copy(part, part, sem).wait()

    barrier = pltpu.get_barrier_semaphore()
    for i in range(1, n_grp):
        @pl.when(grp_at(i) > g)
        def _(i=i):
            pl.semaphore_signal(barrier, inc=1, **to_grp(i))

    def greet(j, carry):
        pl.semaphore_signal(barrier, inc=1, **to_dev(j))
        return carry
    lax.fori_loop(1, n_dev - d, greet, 0)

    load_ids = pltpu.make_async_copy(ids_hbm, ids_buf.at[g], ids_sem)
    load_ids.start()
    load_table = pltpu.make_async_copy(table_ref, tbl, tbl_sem)
    load_w = pltpu.make_async_copy(w_ref, wbuf, w_sem)
    load_hidden = pltpu.make_async_copy(hidden_hbm, hidden_ref, hidden_sem)
    load_gain = pltpu.make_async_copy(gain_hbm, gain_ref, gain_sem)

    part = rows // PIECES
    pieces = [(l, p) for l in range(layer_share) for p in range(PIECES)]

    def tab_copy(i, l, p):
        gp = grp_at(i)
        return pltpu.make_async_remote_copy(
            src_ref=table_ref.at[l, pl.ds(pl.multiple_of(gp * rows + p * part, part), part), :],
            dst_ref=served_ref.at[
                pl.ds(p * part, part),
                pl.ds(pl.multiple_of((g * layer_share + l) * width, width), width),
            ],
            send_sem=tab_ss, recv_sem=tab_rs, **to_grp(i),
        )

    cuts = [1] + [len(pieces) * s // 16 for s in SPLIT] + [len(pieces)]

    def start_pieces(k):
        for l, p in pieces[cuts[k]:cuts[k + 1]] if k <= len(SPLIT) else ():
            for i in range(n_grp - 1, 0, -1):
                tab_copy(i, l, p).start()

    def own_copy(l):
        return pltpu.make_async_copy(
            table_ref.at[l, pl.ds(pl.multiple_of(g * rows, rows), rows), :],
            served_ref.at[:, pl.ds(pl.multiple_of((g * layer_share + l) * width, width), width)],
            own_sem,
        )

    def ids_copy(i):
        return pltpu.make_async_remote_copy(
            src_ref=ids_buf.at[g], dst_ref=ids_buf.at[g],
            send_sem=ids_ss, recv_sem=ids_rs, **to_grp(i),
        )

    @pl.when(g + d > 0)
    def _():
        pl.semaphore_wait(barrier, g + d)
    for i in range(1, n_grp):
        @pl.when(grp_at(i) < g)
        def _(i=i):
            pl.semaphore_signal(in_grp.at[back(i)], inc=1, **to_grp(i))

    def reply(j, carry):
        pl.semaphore_signal(in_dev, inc=1, **to_dev(j))
        return carry
    lax.fori_loop(n_dev - d, n_dev, reply, 0)

    load_ids.wait()
    for i in range(1, n_grp):
        @pl.when(grp_at(i) > g)
        def _(i=i):
            pl.semaphore_wait(in_grp.at[i], 1)
        ids_copy(i).start()
        l, p = pieces[0]
        tab_copy(i, l, p).start()
    start_pieces(0)
    load_table.start()
    for l in range(layer_share):
        own_copy(l).start()

    lane = lax.broadcasted_iota(jnp.int32, (LANES, LANES), 1).astype(f32)
    sub = lax.broadcasted_iota(jnp.int32, (LANES, LANES), 0).astype(f32)
    block_id = lax.broadcasted_iota(jnp.int32, (blocks, LANES), 0).astype(f32)
    base = (d * cap).astype(f32)

    def owner_of(v):
        return jnp.floor((v + 0.5) * (1.0 / rows))

    def ask_for(o, req, row):
        gp = grp_at(o)
        id_row = [ids_buf[gp, h:h + 1, :].astype(f32) for h in range(halves)]
        id_col = [column(v) for v in id_row]
        own_row = [owner_of(v) for v in id_row]
        own_col = [owner_of(v) for v in id_col]
        slot_col = []
        for h in range(halves):
            earlier = jnp.zeros((LANES, LANES), f32)
            for k in range(h + 1):
                same = own_col[h] == own_row[k]
                if k == h:
                    same = same & (lane < sub)
                earlier = earlier + jnp.where(same, 1.0, 0.0)
            slot_col.append(jnp.sum(earlier, axis=1, keepdims=True))
            want[o, h] = own_col[h] * cap + slot_col[h]
        chooser = jnp.concatenate(
            [jnp.where(own_row[h] == block_id, 1.0, 0.0).astype(bf16) for h in range(halves)], axis=1
        )
        for r in range(groups):
            high, low = [], []
            for h in range(halves):
                at_slot = slot_col[h] == lane + (r * LANES) - base
                local = id_col[h] - own_col[h] * rows
                hi = jnp.floor(local * (1.0 / 256.0))
                high.append(jnp.where(at_slot, hi, 0.0).astype(bf16))
                low.append(jnp.where(at_slot, local - hi * 256.0 + 1.0, 0.0).astype(bf16))
            ask = jnp.dot(chooser, jnp.concatenate(high, axis=0), preferred_element_type=f32) * 256.0
            ask = ask + jnp.dot(chooser, jnp.concatenate(low, axis=0), preferred_element_type=f32)
            req[:, row:row + n_grp, r * LANES:(r + 1) * LANES] = (
                ask.reshape(n_dev, n_grp, LANES)
            )

    def req_copy(k, j):
        return pltpu.make_async_remote_copy(
            src_ref=req_send[k].at[dev_at(j)], dst_ref=req_buf[k].at[d],
            send_sem=req_ss.at[k], recv_sem=req_rs.at[k], **to_dev(j),
        )

    def start_req(k):
        def body(j, carry):
            req_copy(k, j).start()
            return carry
        lax.fori_loop(1, n_dev, body, 0)
        req_buf[k][d] = req_send[k][d]

    def take_req(k):
        drain(req_buf[k].at[pl.ds(0, n_dev - 1)], req_rs.at[k])
        total = req_buf[k][0]
        for a in range(1, n_dev):
            total = total + req_buf[k][a]
        return total

    load_w.start()
    load_hidden.start()
    load_gain.start()
    ask_for(0, req_send[0], 0)
    @pl.when(d < n_dev - 1)
    def _():
        pl.semaphore_wait(in_dev, n_dev - 1 - d)
    start_req(0)
    drain(ids_buf.at[pl.ds(0, n_grp - 1)], ids_rs)
    for o in range(1, n_grp):
        ask_for(o, req_send[1], (o - 1) * n_grp)
    start_req(1)

    first = max(1, n_grp * OWN_FIRST // 4)
    wide = layer_share * width
    both = [o for o in range(n_grp - 1, 0, -1) if o // 2 and o % 2]
    single = [o for o in range(1, n_grp) if o not in both]
    units = [(0, 0, first, 0, wide)] + [(o, 0, n_grp, 0, wide) for o in both]
    steps = [[u] for u in range(len(units))]
    for c0 in (0, wide // 2):
        steps.append(list(range(len(units), len(units) + len(single))))
        units += [(o, 0, n_grp, c0, c0 + wide // 2) for o in single]
    steps.append([len(units)])
    units.append((0, first, n_grp, 0, wide))
    last = len(steps) - 1

    def z_copy(u, j):
        o, lo, hi, c0, c1 = units[u]
        span = (hi - lo) * cap
        return pltpu.make_async_remote_copy(
            src_ref=send.at[o, dev_at(j), lo * cap:hi * cap, c0:c1],
            dst_ref=recv.at[grp_at(o), pl.ds(pl.multiple_of(d * slots + lo * cap, cap), span), c0:c1],
            send_sem=z_ss, recv_sem=z_rs.at[u], **to_dev(j),
        )

    def start_rows(s):
        def body(j, carry):
            for u in steps[s]:
                z_copy(u, j).start()
            return carry
        lax.fori_loop(1, n_dev, body, 0)

    spread = LANES // cap
    total = take_req(0)
    for b in range(n_grp):
        merged[0, b] = total[b:b + 1, :]
    load_table.wait()
    looked = set()
    for f, members in enumerate(steps):
        if f == 1:
            total = take_req(1)
            for k in range(n_grp, n_grp * n_grp):
                merged[k // n_grp, k % n_grp] = total[k - n_grp:k - n_grp + 1, :]

        for o, lo, hi in [units[u][:3] for u in members]:
            if (o, lo) in looked:
                continue
            looked.add((o, lo))

            def block(b, carry, o=o):
                at = pl.multiple_of(b * cap, cap)
                for r in range(groups):
                    wanted = column(merged[o, b, :, r * LANES:(r + 1) * LANES]) - (lane + 1.0)
                    hit = jnp.concatenate(
                        [(wanted == float(c * LANES)).astype(f32) for c in range(rows // LANES)], axis=1
                    ).astype(bf16)
                    for l in range(layer_share):
                        found = jnp.dot(
                            hit, tbl[l, pl.ds(pl.multiple_of(b * rows, rows), rows), :],
                            preferred_element_type=f32,
                        ).astype(bf16)
                        send[o, r * spread:(r + 1) * spread, pl.ds(at, cap), l * width:(l + 1) * width] = (
                            found.reshape(spread, cap, width)
                        )
                return carry
            lax.fori_loop(lo, hi, block, 0)
            recv[grp_at(o), pl.ds(pl.multiple_of(d * slots + lo * cap, cap), (hi - lo) * cap), :] = (
                send[o, d, lo * cap:hi * cap]
            )
        if f < AHEAD:
            start_rows(f)

    load_w.wait()
    load_hidden.wait()
    load_gain.wait()

    def project(l):
        proj = jnp.dot(hidden_ref[...], wbuf[:, l * width:(l + 1) * width], preferred_element_type=f32)
        mean_sq = jnp.mean(proj * proj, axis=-1, keepdims=True)
        return proj / jnp.sqrt(mean_sq + 1e-06) * gain_ref[...]

    for l in range(layers):
        mix[:, l, :] = project(l)

    def e_copy(u):
        o, _, _, c0, c1 = units[u]
        return pltpu.make_async_remote_copy(
            src_ref=esend.at[o, :, c0:c1], dst_ref=erecv.at[g, :, c0:c1],
            send_sem=e_ss, recv_sem=e_rs.at[u], **to_grp(o),
        )

    def take_rows(f):
        for u in steps[f]:
            o, lo, hi, c0, c1 = units[u]
            drain(recv.at[0, pl.ds(0, (n_dev - 1) * (hi - lo) * cap), c0:c1], z_rs.at[u])

    def pickers(o):
        made = []
        for t in range(halves):
            mine = want[o, t] - lane
            made.append(jnp.concatenate(
                [(mine == float(c * LANES)).astype(f32) for c in range(all_slots // LANES)], axis=1
            ).astype(bf16))
        return made

    def pick(u, dst, at):
        o, _, _, c0, c1 = units[u]
        for t, picker in enumerate(pickers(o)):
            dst[at, t * LANES:(t + 1) * LANES, c0:c1] = jnp.dot(
                picker, recv[grp_at(o), :, c0:c1], preferred_element_type=f32
            ).astype(bf16)

    def add_rows(source, u):
        c0, c1 = units[u][3:]
        for a in range(n_grp):
            @pl.when(source == a)
            def _(a=a):
                for k in range(layer_share):
                    lo, hi = max(c0, k * width), min(c1, (k + 1) * width)
                    if lo < hi:
                        l, at = a * layer_share + k, slice(lo - k * width, hi - k * width)
                        emb = erecv[a, :, lo:hi].astype(f32)
                        mix[:, l, at] = (mix[:, l, at] + math.sqrt(width) * emb) / math.sqrt(2.0)

    def add_from_peer(u):
        e_copy(u).wait_recv()
        add_rows(grp_at(back(units[u][0])), u)

    take_rows(0)
    if AHEAD <= last:
        start_rows(AHEAD)
    for f in range(1, last):
        take_rows(f)
        if f + AHEAD <= last:
            start_rows(f + AHEAD)
        for u in steps[f]:
            pick(u, esend, units[u][0])
            e_copy(u).start()
        start_pieces(f)

    for f in range(1, last - 1):
        for u in steps[f]:
            add_from_peer(u)
    take_rows(last)
    pick(steps[last][0], erecv, g)
    add_rows(g, steps[last][0])
    for u in steps[last - 1]:
        add_from_peer(u)
    out_ref[...] = mix[...].astype(bf16)

    drain(served_ref.at[:, pl.ds(0, wide)], own_sem)
    drain(ids_buf.at[pl.ds(0, n_grp - 1)], ids_ss)
    for k in range(2):
        drain(req_send[k].at[pl.ds(0, n_dev - 1)], req_ss.at[k])
    drain(send.at[:, pl.ds(0, n_dev - 1)], z_ss)
    drain(esend.at[pl.ds(0, n_grp - 1)], e_ss)
    drain(served_ref.at[:, pl.ds(0, (n_grp - 1) * wide)], tab_ss)
    drain(served_ref.at[:, pl.ds(0, (n_grp - 1) * wide)], tab_rs)


def put_out(served_ref, mixed_ref, served_hbm, mixed_hbm, sems):
    parts = sems.shape[0] - 1
    span = served_ref.shape[0] // parts
    copies = [
        pltpu.make_async_copy(
            served_ref.at[pl.ds(k * span, span), :], served_hbm.at[pl.ds(k * span, span), :], sems.at[k]
        )
        for k in range(parts)
    ]
    copies.append(pltpu.make_async_copy(mixed_ref, mixed_hbm, sems.at[parts]))
    for copy in copies:
        copy.start()
    for copy in copies:
        copy.wait()


def on_device(table, token_ids, hidden, w_proj, norm_gain):
    n_grp = lax.axis_size("grp")
    n_dev = lax.axis_size("dev")
    layer_share, vocab_share, width = table.shape
    layers = layer_share * n_grp
    tok = token_ids.shape[0]
    rows = vocab_share // n_grp
    blocks = n_grp * n_dev
    cap = -(-max(2, 2 * tok // blocks) // 16) * 16
    slots = n_grp * cap
    lanes = n_dev * cap
    assert n_grp % 2 == 0 and lanes % LANES == 0 and tok % LANES == 0 and rows % LANES == 0
    wide = layer_share * width

    vmem = pl.BlockSpec(memory_space=pltpu.VMEM)
    hbm = pl.BlockSpec(memory_space=pltpu.HBM)
    dma = pltpu.SemaphoreType.DMA
    bf16 = jnp.bfloat16
    f32 = jnp.float32
    served, mixed = pl.pallas_call(
        functools.partial(exchange, n_grp, n_dev, cap),
        out_shape=(
            pltpu.VMEM((rows, layers * width), bf16),
            pltpu.VMEM((tok, layers, width), bf16),
        ),
        in_specs=[hbm] * 5,
        out_specs=(vmem, vmem),
        scratch_shapes=[
            pltpu.VMEM((n_grp, tok // LANES, LANES), jnp.int32),
            pltpu.VMEM(hidden.shape, bf16),
            pltpu.VMEM((1, width), f32),
            pltpu.VMEM(table.shape, bf16),
            pltpu.VMEM(w_proj.shape, bf16),
            pltpu.VMEM((n_grp, tok // LANES, LANES, LANES), f32),
            pltpu.VMEM((n_dev, n_grp, lanes), f32),
            pltpu.VMEM((n_dev, (n_grp - 1) * n_grp, lanes), f32),
            pltpu.VMEM((n_dev, n_grp, lanes), f32),
            pltpu.VMEM((n_dev, (n_grp - 1) * n_grp, lanes), f32),
            pltpu.VMEM((n_grp, n_grp, 1, lanes), f32),
            pltpu.VMEM((n_grp, n_dev, slots, wide), bf16),
            pltpu.VMEM((n_grp, n_dev * slots, wide), bf16),
            pltpu.VMEM((n_grp, tok, wide), bf16),
            pltpu.VMEM((n_grp, tok, wide), bf16),
            pltpu.VMEM((tok, layers, width), f32),
            dma, dma,
            dma((2,)), dma((2,)),
            dma, dma,
            dma, dma((2 * n_grp,)),
            dma, dma((2 * n_grp,)),
            pltpu.SemaphoreType.REGULAR((n_grp,)), pltpu.SemaphoreType.REGULAR,
            dma, dma, dma, dma, dma, dma,
        ],
        compiler_params=pltpu.CompilerParams(
            collective_id=0, has_side_effects=True, vmem_limit_bytes=58 * 2**20
        ),
        name="exchange",
    )(token_ids.reshape(tok // LANES, LANES), hidden, norm_gain.reshape(1, width), table, w_proj)
    served, mixed = pl.pallas_call(
        put_out,
        out_shape=(
            jax.ShapeDtypeStruct(served.shape, bf16),
            jax.ShapeDtypeStruct(mixed.shape, bf16),
        ),
        in_specs=[vmem, vmem],
        out_specs=(hbm, hbm),
        scratch_shapes=[dma((9,))],
        compiler_params=pltpu.CompilerParams(vmem_limit_bytes=2 * 2**20),
        name="put_out",
    )(served, mixed)
    return (served.reshape(1, 1, rows, layers * width), mixed)


def solution(mesh):
    in_specs = (P("grp", "dev", None), P(("grp", "dev")), P(("grp", "dev"), None), P(), P())
    out_specs = (P("dev", "grp", None, None), P(("grp", "dev"), None, None))
    return jax.shard_map(
        on_device, mesh=mesh, in_specs=in_specs, out_specs=out_specs, check_vma=False
    )
```

```python
import functools
import math

import jax
import jax.numpy as jnp
from jax import lax
from jax.experimental import pallas as pl
from jax.experimental.pallas import tpu as pltpu
from jax.sharding import PartitionSpec as P

MESH = pl.DeviceIdType.MESH
LANES = 128
PIECES = 8
SPLIT = (12, 14, 15)
OWN_FIRST = 1
AHEAD = 2


def column(row):
    return jnp.transpose(jnp.broadcast_to(row, (LANES, LANES)))


def exchange(n_grp, n_dev, cap,
             ids_hbm, hidden_hbm, gain_hbm, table_ref, w_ref,
             served_ref, out_ref,
             ids_buf, hidden_ref, gain_ref, tbl, wbuf, want, req_own, req_oth, buf_own, buf_oth, merged,
             send, recv, esend, erecv, mix,
             ids_ss, ids_rs, req_ss, req_rs, tab_ss, tab_rs, z_ss, z_rs, e_ss, e_rs,
             in_grp, in_dev, ids_sem, tbl_sem, w_sem, hidden_sem, gain_sem, own_sem):
    g = lax.axis_index("grp")
    d = lax.axis_index("dev")
    layer_share, vocab_share, width = table_ref.shape
    rows = vocab_share // n_grp
    tok = hidden_ref.shape[0]
    halves = tok // LANES
    layers = layer_share * n_grp
    blocks = n_grp * n_dev
    slots = n_grp * cap
    all_slots = n_dev * slots
    groups = n_dev * cap // LANES
    half_grp = n_grp // 2
    req_send = (req_own, req_oth)
    req_buf = (buf_own, buf_oth)
    f32 = jnp.float32
    bf16 = jnp.bfloat16

    def grp_at(i):
        return lax.rem(g // 2 + i // 2, half_grp) * 2 + lax.rem(g % 2 + i % 2, 2)

    def back(i):
        return ((half_grp - i // 2) % half_grp) * 2 + i % 2

    def dev_at(j):
        return lax.rem(d + j, n_dev)

    def to_grp(i):
        return dict(device_id={"grp": grp_at(i), "dev": d}, device_id_type=MESH)

    def to_dev(j):
        return dict(device_id={"grp": g, "dev": dev_at(j)}, device_id_type=MESH)

    def drain(part, sem):
        pltpu.make_async_copy(part, part, sem).wait()

    high, low = g // 2, g % 2

    def below(i):
        p = grp_at(i)
        return (p // 2 <= high) & (p % 2 <= low)

    def above(i):
        p = grp_at(i)
        return (p // 2 >= high) & (p % 2 >= low)

    barrier = pltpu.get_barrier_semaphore()
    for i in range(1, n_grp):
        @pl.when(above(i))
        def _(i=i):
            pl.semaphore_signal(barrier, inc=1, **to_grp(i))

    def greet(j, carry):
        pl.semaphore_signal(barrier, inc=1, **to_dev(j))
        return carry
    lax.fori_loop(1, n_dev - d, greet, 0)

    load_ids = pltpu.make_async_copy(ids_hbm, ids_buf.at[g], ids_sem)
    load_ids.start()
    load_table = pltpu.make_async_copy(table_ref, tbl, tbl_sem)
    load_w = pltpu.make_async_copy(w_ref, wbuf, w_sem)
    load_hidden = pltpu.make_async_copy(hidden_hbm, hidden_ref, hidden_sem)
    load_gain = pltpu.make_async_copy(gain_hbm, gain_ref, gain_sem)

    part = rows // PIECES
    pieces = [(l, p) for l in range(layer_share) for p in range(PIECES)]

    def tab_copy(i, l, p, at=0, part=part):
        gp = grp_at(i)
        first_row = p * (rows // PIECES) + at
        return pltpu.make_async_remote_copy(
            src_ref=table_ref.at[l, pl.ds(pl.multiple_of(gp * rows + first_row, part), part), :],
            dst_ref=served_ref.at[
                pl.ds(first_row, part),
                pl.ds(pl.multiple_of((g * layer_share + l) * width, width), width),
            ],
            send_sem=tab_ss, recv_sem=tab_rs, **to_grp(i),
        )

    cuts = [1] + [len(pieces) * s // 16 for s in SPLIT] + [len(pieces)]

    def start_pieces(k):
        for l, p in pieces[cuts[k]:cuts[k + 1]] if k <= len(SPLIT) else ():
            for i in range(n_grp - 1, 0, -1):
                tab_copy(i, l, p).start()

    def own_copy(l):
        return pltpu.make_async_copy(
            table_ref.at[l, pl.ds(pl.multiple_of(g * rows, rows), rows), :],
            served_ref.at[:, pl.ds(pl.multiple_of((g * layer_share + l) * width, width), width)],
            own_sem,
        )

    def ids_copy(i):
        return pltpu.make_async_remote_copy(
            src_ref=ids_buf.at[g], dst_ref=ids_buf.at[g],
            send_sem=ids_ss, recv_sem=ids_rs, **to_grp(i),
        )

    @pl.when(g + d > 0)
    def _():
        pl.semaphore_wait(barrier, (high + 1) * (low + 1) - 1 + d)
    for i in range(1, n_grp):
        @pl.when(below(i))
        def _(i=i):
            pl.semaphore_signal(in_grp.at[back(i)], inc=1, **to_grp(i))

    def reply(j, carry):
        pl.semaphore_signal(in_dev, inc=1, **to_dev(j))
        return carry
    lax.fori_loop(n_dev - d, n_dev, reply, 0)

    l, p = pieces[0]
    half = part // 2
    for i in range(1, n_grp):
        @pl.when(below(i))
        def _(i=i):
            tab_copy(i, l, p, 0, half).start()
    load_ids.wait()
    for i in range(1, n_grp):
        @pl.when(jnp.logical_not(below(i)))
        def _(i=i):
            pl.semaphore_wait(in_grp.at[i], 1)
        if i % 2 == 0:
            @pl.when((low == 0) & (high + i // 2 < half_grp))
            def _(i=i):
                pl.semaphore_signal(in_grp.at[i + 1], inc=1, **to_grp(1))
                pl.semaphore_signal(in_grp.at[n_grp - i + 1], inc=1, **to_grp(i))
        ids_copy(i).start()
        @pl.when(jnp.logical_not(below(i)))
        def _(i=i):
            tab_copy(i, l, p, 0, half).start()
        tab_copy(i, l, p, half, half).start()
    start_pieces(0)
    load_table.start()
    for l in range(layer_share):
        own_copy(l).start()

    lane = lax.broadcasted_iota(jnp.int32, (LANES, LANES), 1).astype(f32)
    sub = lax.broadcasted_iota(jnp.int32, (LANES, LANES), 0).astype(f32)
    block_id = lax.broadcasted_iota(jnp.int32, (blocks, LANES), 0).astype(f32)
    base = (d * cap).astype(f32)

    def owner_of(v):
        return jnp.floor((v + 0.5) * (1.0 / rows))

    def ask_for(o, req, row):
        gp = grp_at(o)
        id_row = [ids_buf[gp, h:h + 1, :].astype(f32) for h in range(halves)]
        id_col = [column(v) for v in id_row]
        own_row = [owner_of(v) for v in id_row]
        own_col = [owner_of(v) for v in id_col]
        slot_col = []
        for h in range(halves):
            earlier = jnp.zeros((LANES, LANES), f32)
            for k in range(h + 1):
                same = own_col[h] == own_row[k]
                if k == h:
                    same = same & (lane < sub)
                earlier = earlier + jnp.where(same, 1.0, 0.0)
            slot_col.append(jnp.sum(earlier, axis=1, keepdims=True))
            want[o, h] = own_col[h] * cap + slot_col[h]
        chooser = jnp.concatenate(
            [jnp.where(own_row[h] == block_id, 1.0, 0.0).astype(bf16) for h in range(halves)], axis=1
        )
        for r in range(groups):
            high, low = [], []
            for h in range(halves):
                at_slot = slot_col[h] == lane + (r * LANES) - base
                local = id_col[h] - own_col[h] * rows
                hi = jnp.floor(local * (1.0 / 256.0))
                high.append(jnp.where(at_slot, hi, 0.0).astype(bf16))
                low.append(jnp.where(at_slot, local - hi * 256.0 + 1.0, 0.0).astype(bf16))
            ask = jnp.dot(chooser, jnp.concatenate(high, axis=0), preferred_element_type=f32) * 256.0
            ask = ask + jnp.dot(chooser, jnp.concatenate(low, axis=0), preferred_element_type=f32)
            req[:, row:row + n_grp, r * LANES:(r + 1) * LANES] = (
                ask.reshape(n_dev, n_grp, LANES)
            )

    def req_copy(k, j):
        return pltpu.make_async_remote_copy(
            src_ref=req_send[k].at[dev_at(j)], dst_ref=req_buf[k].at[d],
            send_sem=req_ss.at[k], recv_sem=req_rs.at[k], **to_dev(j),
        )

    def start_req(k):
        def body(j, carry):
            req_copy(k, j).start()
            return carry
        lax.fori_loop(1, n_dev, body, 0)
        req_buf[k][d] = req_send[k][d]

    def take_req(k):
        drain(req_buf[k].at[pl.ds(0, n_dev - 1)], req_rs.at[k])
        total = req_buf[k][0]
        for a in range(1, n_dev):
            total = total + req_buf[k][a]
        return total

    load_w.start()
    load_hidden.start()
    load_gain.start()
    ask_for(0, req_send[0], 0)
    @pl.when(d < n_dev - 1)
    def _():
        pl.semaphore_wait(in_dev, n_dev - 1 - d)
    start_req(0)
    drain(ids_buf.at[pl.ds(0, n_grp - 1)], ids_rs)
    for o in range(1, n_grp):
        ask_for(o, req_send[1], (o - 1) * n_grp)
    start_req(1)

    first = max(1, n_grp * OWN_FIRST // 4)
    wide = layer_share * width
    both = [o for o in range(n_grp - 1, 0, -1) if o // 2 and o % 2]
    single = [o for o in range(1, n_grp) if o not in both]
    units = [(0, 0, first, 0, wide)] + [(o, 0, n_grp, 0, wide) for o in both]
    steps = [[u] for u in range(len(units))]
    for c0 in (0, wide // 2):
        steps.append(list(range(len(units), len(units) + len(single))))
        units += [(o, 0, n_grp, c0, c0 + wide // 2) for o in single]
    steps.append([len(units)])
    units.append((0, first, n_grp, 0, wide))
    last = len(steps) - 1

    def z_copy(u, j):
        o, lo, hi, c0, c1 = units[u]
        span = (hi - lo) * cap
        return pltpu.make_async_remote_copy(
            src_ref=send.at[o, dev_at(j), lo * cap:hi * cap, c0:c1],
            dst_ref=recv.at[grp_at(o), pl.ds(pl.multiple_of(d * slots + lo * cap, cap), span), c0:c1],
            send_sem=z_ss, recv_sem=z_rs.at[u], **to_dev(j),
        )

    def start_rows(s):
        def body(j, carry):
            for u in steps[s]:
                z_copy(u, j).start()
            return carry
        lax.fori_loop(1, n_dev, body, 0)

    spread = LANES // cap
    total = take_req(0)
    for b in range(n_grp):
        merged[0, b] = total[b:b + 1, :]
    load_table.wait()
    looked = set()
    for f, members in enumerate(steps):
        if f == 1:
            total = take_req(1)
            for k in range(n_grp, n_grp * n_grp):
                merged[k // n_grp, k % n_grp] = total[k - n_grp:k - n_grp + 1, :]

        for o, lo, hi in [units[u][:3] for u in members]:
            if (o, lo) in looked:
                continue
            looked.add((o, lo))

            def block(b, carry, o=o):
                at = pl.multiple_of(b * cap, cap)
                for r in range(groups):
                    wanted = column(merged[o, b, :, r * LANES:(r + 1) * LANES]) - (lane + 1.0)
                    hit = jnp.concatenate(
                        [(wanted == float(c * LANES)).astype(f32) for c in range(rows // LANES)], axis=1
                    ).astype(bf16)
                    for l in range(layer_share):
                        found = jnp.dot(
                            hit, tbl[l, pl.ds(pl.multiple_of(b * rows, rows), rows), :],
                            preferred_element_type=f32,
                        ).astype(bf16)
                        send[o, r * spread:(r + 1) * spread, pl.ds(at, cap), l * width:(l + 1) * width] = (
                            found.reshape(spread, cap, width)
                        )
                return carry
            lax.fori_loop(lo, hi, block, 0)
            recv[grp_at(o), pl.ds(pl.multiple_of(d * slots + lo * cap, cap), (hi - lo) * cap), :] = (
                send[o, d, lo * cap:hi * cap]
            )
        if f < AHEAD:
            start_rows(f)

    load_w.wait()
    load_hidden.wait()
    load_gain.wait()

    def project(l):
        proj = jnp.dot(hidden_ref[...], wbuf[:, l * width:(l + 1) * width], preferred_element_type=f32)
        mean_sq = jnp.mean(proj * proj, axis=-1, keepdims=True)
        return proj / jnp.sqrt(mean_sq + 1e-06) * gain_ref[...]

    for l in range(layers):
        mix[:, l, :] = project(l)

    def e_copy(u):
        o, _, _, c0, c1 = units[u]
        return pltpu.make_async_remote_copy(
            src_ref=esend.at[o, :, c0:c1], dst_ref=erecv.at[g, :, c0:c1],
            send_sem=e_ss, recv_sem=e_rs.at[u], **to_grp(o),
        )

    def take_rows(f):
        for u in steps[f]:
            o, lo, hi, c0, c1 = units[u]
            drain(recv.at[0, pl.ds(0, (n_dev - 1) * (hi - lo) * cap), c0:c1], z_rs.at[u])

    def pickers(o):
        made = []
        for t in range(halves):
            mine = want[o, t] - lane
            made.append(jnp.concatenate(
                [(mine == float(c * LANES)).astype(f32) for c in range(all_slots // LANES)], axis=1
            ).astype(bf16))
        return made

    def pick(u, dst, at):
        o, _, _, c0, c1 = units[u]
        for t, picker in enumerate(pickers(o)):
            dst[at, t * LANES:(t + 1) * LANES, c0:c1] = jnp.dot(
                picker, recv[grp_at(o), :, c0:c1], preferred_element_type=f32
            ).astype(bf16)

    def add_rows(source, u):
        c0, c1 = units[u][3:]
        for a in range(n_grp):
            @pl.when(source == a)
            def _(a=a):
                for k in range(layer_share):
                    lo, hi = max(c0, k * width), min(c1, (k + 1) * width)
                    if lo < hi:
                        l, at = a * layer_share + k, slice(lo - k * width, hi - k * width)
                        emb = erecv[a, :, lo:hi].astype(f32)
                        mix[:, l, at] = (mix[:, l, at] + math.sqrt(width) * emb) / math.sqrt(2.0)

    def add_from_peer(u):
        e_copy(u).wait_recv()
        add_rows(grp_at(back(units[u][0])), u)

    take_rows(0)
    if AHEAD <= last:
        start_rows(AHEAD)
    for f in range(1, last):
        take_rows(f)
        if f + AHEAD <= last:
            start_rows(f + AHEAD)
        for u in steps[f]:
            pick(u, esend, units[u][0])
            e_copy(u).start()
        start_pieces(f)

    for f in range(1, last - 1):
        for u in steps[f]:
            add_from_peer(u)
    take_rows(last)
    pick(steps[last][0], erecv, g)
    add_rows(g, steps[last][0])
    for u in steps[last - 1]:
        add_from_peer(u)
    out_ref[...] = mix[...].astype(bf16)

    drain(served_ref.at[:, pl.ds(0, wide)], own_sem)
    drain(ids_buf.at[pl.ds(0, n_grp - 1)], ids_ss)
    for k in range(2):
        drain(req_send[k].at[pl.ds(0, n_dev - 1)], req_ss.at[k])
    drain(send.at[:, pl.ds(0, n_dev - 1)], z_ss)
    drain(esend.at[pl.ds(0, n_grp - 1)], e_ss)
    drain(served_ref.at[:, pl.ds(0, (n_grp - 1) * wide)], tab_ss)
    drain(served_ref.at[:, pl.ds(0, (n_grp - 1) * wide)], tab_rs)


def put_out(served_ref, mixed_ref, served_hbm, mixed_hbm, sems):
    parts = sems.shape[0] - 1
    span = served_ref.shape[0] // parts
    copies = [
        pltpu.make_async_copy(
            served_ref.at[pl.ds(k * span, span), :], served_hbm.at[pl.ds(k * span, span), :], sems.at[k]
        )
        for k in range(parts)
    ]
    copies.append(pltpu.make_async_copy(mixed_ref, mixed_hbm, sems.at[parts]))
    for copy in copies:
        copy.start()
    for copy in copies:
        copy.wait()


def on_device(table, token_ids, hidden, w_proj, norm_gain):
    n_grp = lax.axis_size("grp")
    n_dev = lax.axis_size("dev")
    layer_share, vocab_share, width = table.shape
    layers = layer_share * n_grp
    tok = token_ids.shape[0]
    rows = vocab_share // n_grp
    blocks = n_grp * n_dev
    cap = -(-max(2, 2 * tok // blocks) // 16) * 16
    slots = n_grp * cap
    lanes = n_dev * cap
    assert n_grp % 2 == 0 and lanes % LANES == 0 and tok % LANES == 0 and rows % LANES == 0
    wide = layer_share * width

    vmem = pl.BlockSpec(memory_space=pltpu.VMEM)
    hbm = pl.BlockSpec(memory_space=pltpu.HBM)
    dma = pltpu.SemaphoreType.DMA
    bf16 = jnp.bfloat16
    f32 = jnp.float32
    served, mixed = pl.pallas_call(
        functools.partial(exchange, n_grp, n_dev, cap),
        out_shape=(
            pltpu.VMEM((rows, layers * width), bf16),
            pltpu.VMEM((tok, layers, width), bf16),
        ),
        in_specs=[hbm] * 5,
        out_specs=(vmem, vmem),
        scratch_shapes=[
            pltpu.VMEM((n_grp, tok // LANES, LANES), jnp.int32),
            pltpu.VMEM(hidden.shape, bf16),
            pltpu.VMEM((1, width), f32),
            pltpu.VMEM(table.shape, bf16),
            pltpu.VMEM(w_proj.shape, bf16),
            pltpu.VMEM((n_grp, tok // LANES, LANES, LANES), f32),
            pltpu.VMEM((n_dev, n_grp, lanes), f32),
            pltpu.VMEM((n_dev, (n_grp - 1) * n_grp, lanes), f32),
            pltpu.VMEM((n_dev, n_grp, lanes), f32),
            pltpu.VMEM((n_dev, (n_grp - 1) * n_grp, lanes), f32),
            pltpu.VMEM((n_grp, n_grp, 1, lanes), f32),
            pltpu.VMEM((n_grp, n_dev, slots, wide), bf16),
            pltpu.VMEM((n_grp, n_dev * slots, wide), bf16),
            pltpu.VMEM((n_grp, tok, wide), bf16),
            pltpu.VMEM((n_grp, tok, wide), bf16),
            pltpu.VMEM((tok, layers, width), f32),
            dma, dma,
            dma((2,)), dma((2,)),
            dma, dma,
            dma, dma((2 * n_grp,)),
            dma, dma((2 * n_grp,)),
            pltpu.SemaphoreType.REGULAR((n_grp,)), pltpu.SemaphoreType.REGULAR,
            dma, dma, dma, dma, dma, dma,
        ],
        compiler_params=pltpu.CompilerParams(
            collective_id=0, has_side_effects=True, vmem_limit_bytes=58 * 2**20
        ),
        name="exchange",
    )(token_ids.reshape(tok // LANES, LANES), hidden, norm_gain.reshape(1, width), table, w_proj)
    served, mixed = pl.pallas_call(
        put_out,
        out_shape=(
            jax.ShapeDtypeStruct(served.shape, bf16),
            jax.ShapeDtypeStruct(mixed.shape, bf16),
        ),
        in_specs=[vmem, vmem],
        out_specs=(hbm, hbm),
        scratch_shapes=[dma((9,))],
        compiler_params=pltpu.CompilerParams(vmem_limit_bytes=2 * 2**20),
        name="put_out",
    )(served, mixed)
    return (served.reshape(1, 1, rows, layers * width), mixed)


def solution(mesh):
    in_specs = (P("grp", "dev", None), P(("grp", "dev")), P(("grp", "dev"), None), P(), P())
    out_specs = (P("dev", "grp", None, None), P(("grp", "dev"), None, None))
    return jax.shard_map(
        on_device, mesh=mesh, in_specs=in_specs, out_specs=out_specs, check_vma=False
    )
```

```python
import functools
import math

import jax
import jax.numpy as jnp
from jax import lax
from jax.experimental import pallas as pl
from jax.experimental.pallas import tpu as pltpu
from jax.sharding import PartitionSpec as P

MESH = pl.DeviceIdType.MESH
LANES = 128
PIECES = 8
SPLIT = (13, 14, 15)
OWN_FIRST = 1
AHEAD = 2


def column(row):
    return jnp.transpose(jnp.broadcast_to(row, (LANES, LANES)))


def exchange(n_grp, n_dev, cap,
             ids_hbm, hidden_hbm, gain_hbm, table_ref, w_ref,
             served_ref, out_ref,
             ids_buf, hidden_ref, gain_ref, tbl, wbuf, want, req_own, req_oth, buf_own, buf_oth, merged,
             send, recv, esend, erecv, mix,
             ids_ss, ids_rs, req_ss, req_rs, tab_ss, tab_rs, z_ss, z_rs, e_ss, e_rs,
             in_grp, in_dev, ids_sem, tbl_sem, w_sem, hidden_sem, gain_sem, own_sem):
    g = lax.axis_index("grp")
    d = lax.axis_index("dev")
    layer_share, vocab_share, width = table_ref.shape
    rows = vocab_share // n_grp
    tok = hidden_ref.shape[0]
    halves = tok // LANES
    layers = layer_share * n_grp
    blocks = n_grp * n_dev
    slots = n_grp * cap
    all_slots = n_dev * slots
    groups = n_dev * cap // LANES
    half_grp = n_grp // 2
    req_send = (req_own, req_oth)
    req_buf = (buf_own, buf_oth)
    f32 = jnp.float32
    bf16 = jnp.bfloat16

    def grp_at(i):
        return lax.rem(g // 2 + i // 2, half_grp) * 2 + lax.rem(g % 2 + i % 2, 2)

    def back(i):
        return ((half_grp - i // 2) % half_grp) * 2 + i % 2

    def dev_at(j):
        return lax.rem(d + j, n_dev)

    def to_grp(i):
        return dict(device_id={"grp": grp_at(i), "dev": d}, device_id_type=MESH)

    def to_dev(j):
        return dict(device_id={"grp": g, "dev": dev_at(j)}, device_id_type=MESH)

    def drain(part, sem):
        pltpu.make_async_copy(part, part, sem).wait()

    high, low = g // 2, g % 2

    def below(i):
        p = grp_at(i)
        return (p // 2 <= high) & (p % 2 <= low)

    def above(i):
        p = grp_at(i)
        return (p // 2 >= high) & (p % 2 >= low)

    barrier = pltpu.get_barrier_semaphore()
    for i in range(1, n_grp):
        @pl.when(above(i))
        def _(i=i):
            pl.semaphore_signal(barrier, inc=1, **to_grp(i))

    def greet(j, carry):
        pl.semaphore_signal(barrier, inc=1, **to_dev(j))
        return carry
    lax.fori_loop(1, n_dev - d, greet, 0)

    load_ids = pltpu.make_async_copy(ids_hbm, ids_buf.at[g], ids_sem)
    load_ids.start()
    load_table = pltpu.make_async_copy(table_ref, tbl, tbl_sem)
    load_w = pltpu.make_async_copy(w_ref, wbuf, w_sem)
    load_hidden = pltpu.make_async_copy(hidden_hbm, hidden_ref, hidden_sem)
    load_gain = pltpu.make_async_copy(gain_hbm, gain_ref, gain_sem)

    part = rows // PIECES
    pieces = [(l, p) for l in range(layer_share) for p in range(PIECES)]

    def tab_copy(i, l, p, at=0, part=part):
        gp = grp_at(i)
        first_row = p * (rows // PIECES) + at
        return pltpu.make_async_remote_copy(
            src_ref=table_ref.at[l, pl.ds(pl.multiple_of(gp * rows + first_row, part), part), :],
            dst_ref=served_ref.at[
                pl.ds(first_row, part),
                pl.ds(pl.multiple_of((g * layer_share + l) * width, width), width),
            ],
            send_sem=tab_ss, recv_sem=tab_rs, **to_grp(i),
        )

    cuts = [1] + [len(pieces) * s // 16 for s in SPLIT] + [len(pieces)]

    def start_pieces(k):
        for l, p in pieces[cuts[k]:cuts[k + 1]] if k <= len(SPLIT) else ():
            for i in range(n_grp - 1, 0, -1):
                tab_copy(i, l, p).start()

    def own_copy(l):
        return pltpu.make_async_copy(
            table_ref.at[l, pl.ds(pl.multiple_of(g * rows, rows), rows), :],
            served_ref.at[:, pl.ds(pl.multiple_of((g * layer_share + l) * width, width), width)],
            own_sem,
        )

    def ids_copy(i):
        return pltpu.make_async_remote_copy(
            src_ref=ids_buf.at[g], dst_ref=ids_buf.at[g],
            send_sem=ids_ss, recv_sem=ids_rs, **to_grp(i),
        )

    @pl.when(g + d > 0)
    def _():
        pl.semaphore_wait(barrier, (high + 1) * (low + 1) - 1 + d)
    for i in range(1, n_grp):
        @pl.when(below(i))
        def _(i=i):
            pl.semaphore_signal(in_grp.at[back(i)], inc=1, **to_grp(i))

    def reply(j, carry):
        pl.semaphore_signal(in_dev, inc=1, **to_dev(j))
        return carry
    lax.fori_loop(n_dev - d, n_dev, reply, 0)

    l, p = pieces[0]
    half = part // 2
    for i in range(1, n_grp):
        @pl.when(below(i))
        def _(i=i):
            tab_copy(i, l, p, 0, half).start()
    load_ids.wait()
    for i in range(1, n_grp):
        @pl.when(jnp.logical_not(below(i)))
        def _(i=i):
            pl.semaphore_wait(in_grp.at[i], 1)
        if i % 2 == 0:
            @pl.when((low == 0) & (high + i // 2 < half_grp))
            def _(i=i):
                pl.semaphore_signal(in_grp.at[i + 1], inc=1, **to_grp(1))
                pl.semaphore_signal(in_grp.at[n_grp - i + 1], inc=1, **to_grp(i))
        ids_copy(i).start()
        @pl.when(jnp.logical_not(below(i)))
        def _(i=i):
            tab_copy(i, l, p, 0, half).start()
        tab_copy(i, l, p, half, half).start()
    start_pieces(0)
    load_table.start()
    for l in range(layer_share):
        own_copy(l).start()

    lane = lax.broadcasted_iota(jnp.int32, (LANES, LANES), 1).astype(f32)
    sub = lax.broadcasted_iota(jnp.int32, (LANES, LANES), 0).astype(f32)
    block_id = lax.broadcasted_iota(jnp.int32, (blocks, LANES), 0).astype(f32)
    base = (d * cap).astype(f32)

    def owner_of(v):
        return jnp.floor((v + 0.5) * (1.0 / rows))

    def ask_for(o, req, row):
        gp = grp_at(o)
        id_row = [ids_buf[gp, h:h + 1, :].astype(f32) for h in range(halves)]
        id_col = [column(v) for v in id_row]
        own_row = [owner_of(v) for v in id_row]
        own_col = [owner_of(v) for v in id_col]
        slot_col = []
        for h in range(halves):
            earlier = jnp.zeros((LANES, LANES), f32)
            for k in range(h + 1):
                same = own_col[h] == own_row[k]
                if k == h:
                    same = same & (lane < sub)
                earlier = earlier + jnp.where(same, 1.0, 0.0)
            slot_col.append(jnp.sum(earlier, axis=1, keepdims=True))
            want[o, h] = own_col[h] * cap + slot_col[h]
        chooser = jnp.concatenate(
            [jnp.where(own_row[h] == block_id, 1.0, 0.0).astype(bf16) for h in range(halves)], axis=1
        )
        for r in range(groups):
            high, low = [], []
            for h in range(halves):
                at_slot = slot_col[h] == lane + (r * LANES) - base
                local = id_col[h] - own_col[h] * rows
                hi = jnp.floor(local * (1.0 / 256.0))
                high.append(jnp.where(at_slot, hi, 0.0).astype(bf16))
                low.append(jnp.where(at_slot, local - hi * 256.0 + 1.0, 0.0).astype(bf16))
            ask = jnp.dot(chooser, jnp.concatenate(high, axis=0), preferred_element_type=f32) * 256.0
            ask = ask + jnp.dot(chooser, jnp.concatenate(low, axis=0), preferred_element_type=f32)
            req[:, row:row + n_grp, r * LANES:(r + 1) * LANES] = (
                ask.reshape(n_dev, n_grp, LANES)
            )

    def req_copy(k, j):
        return pltpu.make_async_remote_copy(
            src_ref=req_send[k].at[dev_at(j)], dst_ref=req_buf[k].at[d],
            send_sem=req_ss.at[k], recv_sem=req_rs.at[k], **to_dev(j),
        )

    def start_req(k):
        def body(j, carry):
            req_copy(k, j).start()
            return carry
        lax.fori_loop(1, n_dev, body, 0)
        req_buf[k][d] = req_send[k][d]

    def take_req(k):
        drain(req_buf[k].at[pl.ds(0, n_dev - 1)], req_rs.at[k])
        total = req_buf[k][0]
        for a in range(1, n_dev):
            total = total + req_buf[k][a]
        return total

    load_w.start()
    load_hidden.start()
    load_gain.start()
    ask_for(0, req_send[0], 0)
    @pl.when(d < n_dev - 1)
    def _():
        pl.semaphore_wait(in_dev, n_dev - 1 - d)
    start_req(0)
    drain(ids_buf.at[pl.ds(0, n_grp - 1)], ids_rs)
    for o in range(1, n_grp):
        ask_for(o, req_send[1], (o - 1) * n_grp)
    start_req(1)

    first = max(1, n_grp * OWN_FIRST // 4)
    wide = layer_share * width
    both = [o for o in range(n_grp - 1, 0, -1) if o // 2 and o % 2]
    single = [o for o in range(1, n_grp) if o not in both]
    units = [(0, 0, first, 0, wide)] + [(o, 0, n_grp, 0, wide) for o in both]
    steps = [[u] for u in range(len(units))]
    for c0 in (0, wide // 2):
        steps.append(list(range(len(units), len(units) + len(single))))
        units += [(o, 0, n_grp, c0, c0 + wide // 2) for o in single]
    steps.append([len(units)])
    units.append((0, first, n_grp, 0, wide))
    last = len(steps) - 1

    def z_copy(u, j):
        o, lo, hi, c0, c1 = units[u]
        span = (hi - lo) * cap
        return pltpu.make_async_remote_copy(
            src_ref=send.at[o, dev_at(j), lo * cap:hi * cap, c0:c1],
            dst_ref=recv.at[grp_at(o), pl.ds(pl.multiple_of(d * slots + lo * cap, cap), span), c0:c1],
            send_sem=z_ss, recv_sem=z_rs.at[u], **to_dev(j),
        )

    def start_rows(s):
        def body(j, carry):
            for u in steps[s]:
                z_copy(u, j).start()
            return carry
        lax.fori_loop(1, n_dev, body, 0)

    spread = LANES // cap
    total = take_req(0)
    for b in range(n_grp):
        merged[0, b] = total[b:b + 1, :]
    load_table.wait()
    looked = set()
    for f, members in enumerate(steps):
        if f == 1:
            total = take_req(1)
            for k in range(n_grp, n_grp * n_grp):
                merged[k // n_grp, k % n_grp] = total[k - n_grp:k - n_grp + 1, :]

        for o, lo, hi in [units[u][:3] for u in members]:
            if (o, lo) in looked:
                continue
            looked.add((o, lo))

            def block(b, carry, o=o):
                at = pl.multiple_of(b * cap, cap)
                for r in range(groups):
                    wanted = column(merged[o, b, :, r * LANES:(r + 1) * LANES]) - (lane + 1.0)
                    hit = jnp.concatenate(
                        [(wanted == float(c * LANES)).astype(f32) for c in range(rows // LANES)], axis=1
                    ).astype(bf16)
                    for l in range(layer_share):
                        found = jnp.dot(
                            hit, tbl[l, pl.ds(pl.multiple_of(b * rows, rows), rows), :],
                            preferred_element_type=f32,
                        ).astype(bf16)
                        send[o, r * spread:(r + 1) * spread, pl.ds(at, cap), l * width:(l + 1) * width] = (
                            found.reshape(spread, cap, width)
                        )
                return carry
            lax.fori_loop(lo, hi, block, 0)
            recv[grp_at(o), pl.ds(pl.multiple_of(d * slots + lo * cap, cap), (hi - lo) * cap), :] = (
                send[o, d, lo * cap:hi * cap]
            )
        if f < AHEAD:
            start_rows(f)

    load_w.wait()
    load_hidden.wait()
    load_gain.wait()

    def project(l):
        proj = jnp.dot(hidden_ref[...], wbuf[:, l * width:(l + 1) * width], preferred_element_type=f32)
        mean_sq = jnp.mean(proj * proj, axis=-1, keepdims=True)
        return proj / jnp.sqrt(mean_sq + 1e-06) * gain_ref[...]

    for l in range(layers):
        mix[:, l, :] = project(l)

    def e_copy(u):
        o, _, _, c0, c1 = units[u]
        return pltpu.make_async_remote_copy(
            src_ref=esend.at[o, :, c0:c1], dst_ref=erecv.at[g, :, c0:c1],
            send_sem=e_ss, recv_sem=e_rs.at[u], **to_grp(o),
        )

    def take_rows(f):
        for u in steps[f]:
            o, lo, hi, c0, c1 = units[u]
            drain(recv.at[0, pl.ds(0, (n_dev - 1) * (hi - lo) * cap), c0:c1], z_rs.at[u])

    def pickers(o):
        made = []
        for t in range(halves):
            mine = want[o, t] - lane
            made.append(jnp.concatenate(
                [(mine == float(c * LANES)).astype(f32) for c in range(all_slots // LANES)], axis=1
            ).astype(bf16))
        return made

    def pick(u, dst, at):
        o, _, _, c0, c1 = units[u]
        for t, picker in enumerate(pickers(o)):
            dst[at, t * LANES:(t + 1) * LANES, c0:c1] = jnp.dot(
                picker, recv[grp_at(o), :, c0:c1], preferred_element_type=f32
            ).astype(bf16)

    def add_rows(source, u):
        c0, c1 = units[u][3:]
        for a in range(n_grp):
            @pl.when(source == a)
            def _(a=a):
                for k in range(layer_share):
                    lo, hi = max(c0, k * width), min(c1, (k + 1) * width)
                    if lo < hi:
                        l, at = a * layer_share + k, slice(lo - k * width, hi - k * width)
                        emb = erecv[a, :, lo:hi].astype(f32)
                        mix[:, l, at] = (mix[:, l, at] + math.sqrt(width) * emb) / math.sqrt(2.0)

    def add_from_peer(u):
        e_copy(u).wait_recv()
        add_rows(grp_at(back(units[u][0])), u)

    take_rows(0)
    if AHEAD <= last:
        start_rows(AHEAD)
    for f in range(1, last):
        take_rows(f)
        if f + AHEAD <= last:
            start_rows(f + AHEAD)
        for u in steps[f]:
            pick(u, esend, units[u][0])
            e_copy(u).start()
        start_pieces(f)

    for f in range(1, last - 1):
        for u in steps[f]:
            add_from_peer(u)
    take_rows(last)
    pick(steps[last][0], erecv, g)
    add_rows(g, steps[last][0])
    for u in steps[last - 1]:
        add_from_peer(u)
    out_ref[...] = mix[...].astype(bf16)

    drain(served_ref.at[:, pl.ds(0, wide)], own_sem)
    drain(ids_buf.at[pl.ds(0, n_grp - 1)], ids_ss)
    for k in range(2):
        drain(req_send[k].at[pl.ds(0, n_dev - 1)], req_ss.at[k])
    drain(send.at[:, pl.ds(0, n_dev - 1)], z_ss)
    drain(esend.at[pl.ds(0, n_grp - 1)], e_ss)
    drain(served_ref.at[:, pl.ds(0, (n_grp - 1) * wide)], tab_ss)
    drain(served_ref.at[:, pl.ds(0, (n_grp - 1) * wide)], tab_rs)


def put_out(served_ref, mixed_ref, served_hbm, mixed_hbm, sems):
    parts = sems.shape[0] - 1
    span = served_ref.shape[0] // parts
    copies = [
        pltpu.make_async_copy(
            served_ref.at[pl.ds(k * span, span), :], served_hbm.at[pl.ds(k * span, span), :], sems.at[k]
        )
        for k in range(parts)
    ]
    copies.append(pltpu.make_async_copy(mixed_ref, mixed_hbm, sems.at[parts]))
    for copy in copies:
        copy.start()
    for copy in copies:
        copy.wait()


def on_device(table, token_ids, hidden, w_proj, norm_gain):
    n_grp = lax.axis_size("grp")
    n_dev = lax.axis_size("dev")
    layer_share, vocab_share, width = table.shape
    layers = layer_share * n_grp
    tok = token_ids.shape[0]
    rows = vocab_share // n_grp
    blocks = n_grp * n_dev
    cap = -(-max(2, 2 * tok // blocks) // 16) * 16
    slots = n_grp * cap
    lanes = n_dev * cap
    assert n_grp % 2 == 0 and lanes % LANES == 0 and tok % LANES == 0 and rows % LANES == 0
    wide = layer_share * width

    vmem = pl.BlockSpec(memory_space=pltpu.VMEM)
    hbm = pl.BlockSpec(memory_space=pltpu.HBM)
    dma = pltpu.SemaphoreType.DMA
    bf16 = jnp.bfloat16
    f32 = jnp.float32
    served, mixed = pl.pallas_call(
        functools.partial(exchange, n_grp, n_dev, cap),
        out_shape=(
            pltpu.VMEM((rows, layers * width), bf16),
            pltpu.VMEM((tok, layers, width), bf16),
        ),
        in_specs=[hbm] * 5,
        out_specs=(vmem, vmem),
        scratch_shapes=[
            pltpu.VMEM((n_grp, tok // LANES, LANES), jnp.int32),
            pltpu.VMEM(hidden.shape, bf16),
            pltpu.VMEM((1, width), f32),
            pltpu.VMEM(table.shape, bf16),
            pltpu.VMEM(w_proj.shape, bf16),
            pltpu.VMEM((n_grp, tok // LANES, LANES, LANES), f32),
            pltpu.VMEM((n_dev, n_grp, lanes), f32),
            pltpu.VMEM((n_dev, (n_grp - 1) * n_grp, lanes), f32),
            pltpu.VMEM((n_dev, n_grp, lanes), f32),
            pltpu.VMEM((n_dev, (n_grp - 1) * n_grp, lanes), f32),
            pltpu.VMEM((n_grp, n_grp, 1, lanes), f32),
            pltpu.VMEM((n_grp, n_dev, slots, wide), bf16),
            pltpu.VMEM((n_grp, n_dev * slots, wide), bf16),
            pltpu.VMEM((n_grp, tok, wide), bf16),
            pltpu.VMEM((n_grp, tok, wide), bf16),
            pltpu.VMEM((tok, layers, width), f32),
            dma, dma,
            dma((2,)), dma((2,)),
            dma, dma,
            dma, dma((2 * n_grp,)),
            dma, dma((2 * n_grp,)),
            pltpu.SemaphoreType.REGULAR((n_grp,)), pltpu.SemaphoreType.REGULAR,
            dma, dma, dma, dma, dma, dma,
        ],
        compiler_params=pltpu.CompilerParams(
            collective_id=0, has_side_effects=True, vmem_limit_bytes=58 * 2**20
        ),
        name="exchange",
    )(token_ids.reshape(tok // LANES, LANES), hidden, norm_gain.reshape(1, width), table, w_proj)
    served, mixed = pl.pallas_call(
        put_out,
        out_shape=(
            jax.ShapeDtypeStruct(served.shape, bf16),
            jax.ShapeDtypeStruct(mixed.shape, bf16),
        ),
        in_specs=[vmem, vmem],
        out_specs=(hbm, hbm),
        scratch_shapes=[dma((9,))],
        compiler_params=pltpu.CompilerParams(vmem_limit_bytes=2 * 2**20),
        name="put_out",
    )(served, mixed)
    return (served.reshape(1, 1, rows, layers * width), mixed)


def solution(mesh):
    in_specs = (P("grp", "dev", None), P(("grp", "dev")), P(("grp", "dev"), None), P(), P())
    out_specs = (P("dev", "grp", None, None), P(("grp", "dev"), None, None))
    return jax.shard_map(
        on_device, mesh=mesh, in_specs=in_specs, out_specs=out_specs, check_vma=False
    )
```
